32 devices in a mesh: shots: 1, gx: 32 (over z, y, x, core), gy: 1.
Axes of the slice: x: 2, y: 2, z: 4, core: 2. Of those that a mesh axis runs over, the one named last changes fastest.
Arguments:
- pressure: float32 [128, 256, 128], P(None, ('shots', 'gx'), 'gy'), may hold values from -6 to 6
- pressure_prior: float32 [128, 256, 128], P(None, ('shots', 'gx'), 'gy'), may hold values from -6 to 6
- courant_square: bfloat16 [128, 256, 128], P(None, 'gx', 'gy'), may hold values from 0.049804688 to 0.1796875
- wavelet: float32 [16], P('shots'), may hold values from -4 to 4
- delay_steps: int32 [256, 128], P(('shots', 'gx'), 'gy'), may hold values from 0 to 7
- source_depth: int32 [256, 128], P(('shots', 'gx'), 'gy'), may hold values from 4 to 31
- receiver_depth: int32 [256, 128], P(('shots', 'gx'), 'gy'), may hold values from 0 to 31
- receiver_field: float32 [128, 256, 128], P(None, ('shots', 'gx'), 'gy'), may hold values from -6 to 6
Outputs:
- pressure_final: float32 [128, 256, 128], P(None, ('shots', 'gx'), 'gy')
- image: float32 [128, 256, 128], P('gx', 'shots', 'gy')
The draws below stay inside these ranges and needn't reach their ends.
All inputs are finite; a program needn't handle non-finite values.
Results may differ from the reference program's by a relative error of at most 0.00035.
Values sent between devices are 32-bit elements; how exact they have to be, the bound alone decides.
A program may use at most 64 MiB of HBM per device.

```python
import math
import jax
import jax.numpy as jnp

STEPS = 8
DMAX = 8
WAVE = 16
NX = 256
NY = 128
NZ = 128


def plant(array, stream_key, low, top_value):
    shape = array.shape
    spot = [jax.random.randint(jax.random.fold_in(stream_key, axis), (), 0, shape[axis]) for axis in range(len(shape))]
    array = array.at[tuple(spot)].set(low)
    longest = shape.index(max(shape))
    spot[longest] = (spot[longest] + 1) % shape[longest]
    return array.at[tuple(spot)].set(top_value)


def block_levels(rng, dims, cuts, low, high):
    def one(axis_at, parts):
        steps = jax.random.uniform(jax.random.fold_in(jax.random.fold_in(rng, 6), axis_at), (parts,), jnp.float32, low / len(cuts), high / len(cuts))
        return jnp.repeat(jnp.exp(steps), dims[axis_at] // parts).reshape((-1,) + (1,) * (len(dims) - axis_at - 1))

    factor_of = one(*cuts[0])
    for cut in cuts[1:]:
        factor_of = factor_of * one(*cut)
    return factor_of


def gaussian(key, dims, scale, most, split=(), kind=jnp.bfloat16):
    gain = block_levels(key, dims, split, -0.22, 0.18) if split else 1.0
    entries = jax.random.normal(key, dims, jnp.float32) * scale * gain
    return jnp.minimum(jnp.maximum(entries, -most), most).astype(kind)


def setup_inputs(seed: int = 0, part: int = 0) -> dict:
    seeds = jax.random.split(jax.random.key(seed), 9)
    own_keys = jax.random.split(jax.random.fold_in(seeds[8], part), 9)
    pressure = gaussian(own_keys[0], (NZ, NX, NY), 1.0, 6.0, ((1, 32),), jnp.float32)
    pressure_prior = gaussian(own_keys[1], (NZ, NX, NY), 1.0, 6.0, ((1, 32),), jnp.float32)
    courant_square = jnp.clip(jnp.exp(math.log(0.1796875) - 1.2831101 * jax.random.uniform(seeds[2], (NZ, NX, NY), jnp.float32) ** block_levels(seeds[2], (NZ, NX, NY), ((1, 32),), -0.2, 0.2)), 0.049804688, 0.1796875).astype(jnp.bfloat16)
    wavelet = gaussian(own_keys[3], (WAVE,), 1.0, 4.0, (), jnp.float32)
    delay_steps = plant(jax.random.randint(own_keys[4], (NX, NY), 0, DMAX), jax.random.fold_in(own_keys[4], 1), 0, DMAX - 1).astype(jnp.int32)
    source_depth = plant(jax.random.randint(own_keys[5], (NX, NY), 4, 32), jax.random.fold_in(own_keys[5], 1), 4, 31).astype(jnp.int32)
    receiver_depth = plant(jax.random.randint(own_keys[6], (NX, NY), 0, NZ // 4), jax.random.fold_in(own_keys[6], 1), 0, (NZ // 4) - 1).astype(jnp.int32)
    receiver_field = gaussian(own_keys[7], (NZ, NX, NY), 1.0, 6.0, ((1, 32),), jnp.float32)
    return dict(pressure=pressure, pressure_prior=pressure_prior, courant_square=courant_square, wavelet=wavelet, delay_steps=delay_steps, source_depth=source_depth, receiver_depth=receiver_depth, receiver_field=receiver_field)


CENTER = -205.0 / 72.0
COEFS = (1.6, -0.2, 8.0 / 315.0, -1.0 / 560.0)


def laplacian(field):
    depth, width, length = field.shape
    padded = jnp.pad(field, 4)
    total = (3.0 * CENTER) * field
    for k in range(1, 5):
        near = padded[4 + k:4 + k + depth, 4:4 + width, 4:4 + length] + padded[4 - k:4 - k + depth, 4:4 + width, 4:4 + length]
        near = near + padded[4:4 + depth, 4 + k:4 + k + width, 4:4 + length] + padded[4:4 + depth, 4 - k:4 - k + width, 4:4 + length]
        near = near + padded[4:4 + depth, 4:4 + width, 4 + k:4 + k + length] + padded[4:4 + depth, 4:4 + width, 4 - k:4 - k + length]
        total = total + COEFS[k - 1] * near
    return total


def injection(step, wavelet, delay_steps, source_depth, depth):
    picks = jnp.arange(wavelet.shape[0], dtype=jnp.int32)
    onehot = (picks[:, None, None] == (delay_steps + step)[None]).astype(wavelet.dtype)
    amplitude = jnp.sum(onehot * wavelet[:, None, None], axis=0)
    levels = jnp.arange(depth, dtype=jnp.int32)[:, None, None]
    return jnp.where(levels == source_depth[None], amplitude[None], jnp.zeros_like(amplitude)[None])


def reference(pressure, pressure_prior, courant_square, wavelet, delay_steps, source_depth, receiver_depth, receiver_field):
    depth = pressure.shape[0]
    coefficient = courant_square.astype(jnp.float32)
    current, prior = pressure, pressure_prior
    for step in range(STEPS):
        nxt = 2.0 * current - prior + coefficient * laplacian(current) + injection(step, wavelet, delay_steps, source_depth, depth)
        prior, current = current, nxt
    levels = jnp.arange(depth, dtype=jnp.int32)[:, None, None]
    masked = jnp.where(levels >= receiver_depth[None], receiver_field, jnp.zeros_like(receiver_field))
    product = current * masked
    padded = jnp.pad(product, ((1, 1), (0, 0), (0, 0)))
    image = 2.0 * product - padded[:-2] - padded[2:]
    return current, image
```

```python
import functools

import jax
import jax.numpy as jnp
from jax import lax
from jax.experimental import pallas as pl
from jax.experimental.pallas import tpu as pltpu
from jax.sharding import PartitionSpec as P

STEPS = 8
REACH = 4
CENTER = -205.0 / 72.0
COEFS = (1.6, -0.2, 8.0 / 315.0, -1.0 / 560.0)
GROUP = 8


def chunks_of(depth):
    quarter = depth // 4
    return ((0, quarter), (depth - quarter, quarter), (quarter, depth - 2 * quarter))


def kernel(
    nx,
    ny,
    pressure,
    prior,
    courant,
    wavelet,
    delay,
    sdepth,
    rdepth,
    receiver,
    final,
    image,
    field,
    side,
    courant_v,
    receiver_v,
    amp,
    product,
    slab,
    weights,
    wave_v,
    delay_v,
    sdepth_v,
    rdepth_v,
    first_sem,
    local_sem,
    send_sem,
    recv_sem,
    side_send,
    side_recv,
    img_send,
    img_recv,
    known,
):
    depth, width, length = pressure.shape
    chunks = chunks_of(depth)
    slab_depth = depth // nx
    me = lax.axis_index("gx")
    mine = lax.axis_index("gy")
    own = pl.ds(REACH, width)

    barrier = pltpu.get_barrier_semaphore()

    def toward(way, far):
        return (me + far, me + far < nx) if way == 0 else (me - far, me >= far)

    if nx > 1:
        for way in (0, 1):
            peer, there = toward(way, 1)

            @pl.when(there)
            def _():
                pl.semaphore_signal(
                    barrier,
                    inc=1,
                    device_id={"gx": peer},
                    device_id_type=pl.DeviceIdType.MESH,
                )

    for j in range(1, ny):
        pl.semaphore_signal(
            barrier,
            inc=1,
            device_id={"gy": lax.rem(mine + j, ny)},
            device_id_type=pl.DeviceIdType.MESH,
        )

    first = [
        pltpu.make_async_copy(
            pressure.at[pl.ds(z, rows), :, :],
            field.at[1, pl.ds(REACH + z, rows), own, :],
            first_sem.at[c],
        )
        for c, (z, rows) in enumerate(chunks)
    ]
    local = [
        pltpu.make_async_copy(prior, field.at[0, pl.ds(REACH, depth), own, :], local_sem.at[0]),
        pltpu.make_async_copy(courant, courant_v, local_sem.at[1]),
        pltpu.make_async_copy(wavelet, wave_v, local_sem.at[2]),
        pltpu.make_async_copy(delay, delay_v, local_sem.at[3]),
        pltpu.make_async_copy(sdepth, sdepth_v, local_sem.at[4]),
        pltpu.make_async_copy(rdepth, rdepth_v, local_sem.at[5]),
        pltpu.make_async_copy(receiver, receiver_v, local_sem.at[6]),
    ]
    for copy in first + local:
        copy.start()

    def span(c):
        z, rows = chunks[c]
        return pl.ds(REACH + z, rows)

    def face(t, c, way):
        source = width if way == 0 else REACH
        target = 0 if way == 0 else REACH + width
        return pltpu.make_async_remote_copy(
            src_ref=field.at[t + 1, span(c), pl.ds(source, REACH), :],
            dst_ref=field.at[t + 1, span(c), pl.ds(target, REACH), :],
            send_sem=send_sem.at[t, c, way],
            recv_sem=recv_sem.at[t, c, way],
            device_id={"gx": lax.rem(me + (1 if way == 0 else nx - 1), nx)},
            device_id_type=pl.DeviceIdType.MESH,
        )

    def flank(t, c, way):
        peer = lax.rem(mine + 1, ny) if way == 0 else lax.rem(mine + ny - 1, ny)
        z, rows = chunks[c]
        return pltpu.make_async_remote_copy(
            src_ref=field.at[t + 1, span(c), own, :],
            dst_ref=side.at[t, way, pl.ds(z, rows), :, :],
            send_sem=side_send.at[t, c, way],
            recv_sem=side_recv.at[t, c, way],
            device_id={"gy": peer},
            device_id_type=pl.DeviceIdType.MESH,
        )

    def each_face(t, c, act, sending):
        if nx > 1:
            for way in (0, 1):
                there = me < nx - 1 if (way == 0) == sending else me > 0

                @pl.when(there)
                def _():
                    act(face(t, c, way))

        if ny > 1:
            for way in (0, 1):
                there = mine < ny - 1 if (way == 0) == sending else mine > 0

                @pl.when(there)
                def _():
                    act(flank(t, c, way))

    def send(t, c):
        each_face(t, c, lambda copy: copy.start(), True)

    def sent(t, c):
        each_face(t, c, lambda copy: copy.wait_send(), True)

    def arrived(t, c):
        each_face(t, c, lambda copy: copy.wait_recv(), False)

    beside = (me > 0).astype(jnp.int32) + (me < nx - 1).astype(jnp.int32)
    if nx > 1 or ny > 1:
        pl.semaphore_wait(barrier, beside + ny - 1)

    for c in range(len(chunks)):
        first[c].wait()
        send(0, c)

    rim = jnp.zeros((REACH, width + 2 * REACH, length), jnp.float32)
    for t in range(STEPS):
        field[t + 1, pl.ds(0, REACH), :, :] = rim
        field[t + 1, pl.ds(REACH + depth, REACH), :, :] = rim

    def clear(at):
        def one(t, carry):
            field[t + 1, pl.ds(REACH, depth), pl.ds(at, REACH), :] = jnp.zeros(
                (depth, REACH, length), jnp.float32
            )
            return carry

        lax.fori_loop(0, STEPS, one, 0)

    @pl.when(me == 0)
    def _():
        clear(0)

    @pl.when(me == nx - 1)
    def _():
        clear(REACH + width)

    if ny > 1:

        def clear_side(k):
            def one(t, carry):
                side[t, k] = jnp.zeros((depth, width, length), jnp.float32)
                return carry

            lax.fori_loop(0, STEPS, one, 0)

        @pl.when(mine == 0)
        def _():
            clear_side(0)

        @pl.when(mine == ny - 1)
        def _():
            clear_side(1)

    product[pl.ds(0, 1), :, :] = jnp.zeros((1, width, length), jnp.float32)
    product[pl.ds(depth + 1, 1), :, :] = jnp.zeros((1, width, length), jnp.float32)

    start = lax.broadcasted_iota(jnp.int32, (length, length), 0)
    gap = jnp.abs(start - lax.broadcasted_iota(jnp.int32, (length, length), 1))
    band = jnp.where(gap == 0, 3.0 * CENTER, 0.0)
    for k in range(1, REACH + 1):
        band = jnp.where(gap == k, COEFS[k - 1], band)
    band_high = band.astype(jnp.bfloat16)
    band_low = (band - band_high.astype(jnp.float32)).astype(jnp.bfloat16)
    weights[...] = jnp.concatenate(
        [
            jnp.concatenate([band_high, band_low], axis=1),
            jnp.concatenate([band_high, jnp.zeros_like(band_low)], axis=1),
        ],
        axis=0,
    )

    for copy in local[:6]:
        copy.wait()
    late = delay_v[...]
    for t in range(STEPS):
        total = jnp.zeros((width, length), jnp.float32)
        for pick in range(wavelet.shape[0]):
            total = total + jnp.where(late + t == pick, wave_v[pick], 0.0)
        amp[t] = total

    lanes = lax.broadcasted_iota(jnp.int32, (width, length), 1)
    origin = sdepth_v[...]

    def along(v):
        tall = v.reshape(GROUP * width, length)
        high = tall.astype(jnp.bfloat16)
        low = (tall - high.astype(jnp.float32)).astype(jnp.bfloat16)
        both = jnp.dot(
            jnp.concatenate([high, low], axis=1), weights[...], preferred_element_type=jnp.float32
        )
        return (both[:, :length] + both[:, length:]).reshape(GROUP, width, length)

    def advance(t, z):
        at = t + 1
        v = field[at, pl.ds(REACH + z, GROUP), own, :]
        old = field[t, pl.ds(REACH + z, GROUP), own, :]
        total = (3.0 * CENTER) * v if ny > 1 else along(v)
        for k in range(1, REACH + 1):
            near = (
                field[at, pl.ds(REACH + z + k, GROUP), own, :]
                + field[at, pl.ds(REACH + z - k, GROUP), own, :]
            )
            near = near + (
                field[at, pl.ds(REACH + z, GROUP), pl.ds(REACH + k, width), :]
                + field[at, pl.ds(REACH + z, GROUP), pl.ds(REACH - k, width), :]
            )
            total = total + COEFS[k - 1] * near
            if ny > 1:
                up = pltpu.roll(v, length - k, 2)
                down = pltpu.roll(v, k, 2)
                low = pltpu.roll(side[t, 0, pl.ds(z, GROUP), :, :], k, 2)
                high = pltpu.roll(side[t, 1, pl.ds(z, GROUP), :, :], length - k, 2)
                up = jnp.where((lanes < length - k)[None], up, high)
                down = jnp.where((lanes >= k)[None], down, low)
                total = total + COEFS[k - 1] * (up + down)
        strength = courant_v[pl.ds(z, GROUP), :, :].astype(jnp.float32)
        levels = lax.broadcasted_iota(jnp.int32, (GROUP, width, length), 0) + z
        shot = jnp.where(levels == origin[None], amp[t][None], 0.0)
        return 2.0 * v - old + strength * total + shot

    reach = []
    while (reach[-1] * 2 if reach else 1) < nx:
        reach.append(reach[-1] * 2 if reach else 1)

    def greet(number):
        for way in (0, 1):
            peer, there = toward(way, reach[number])

            @pl.when(there)
            def _():
                pl.semaphore_signal(
                    known.at[number, way],
                    inc=1,
                    device_id={"gx": peer},
                    device_id_type=pl.DeviceIdType.MESH,
                )

    def greeted(number):
        for way in (0, 1):
            there = toward(1 - way, reach[number])[1]

            @pl.when(there)
            def _():
                pl.semaphore_wait(known.at[number, way], 1)

    def meet(number):
        if number > 0:
            greeted(number - 1)
        greet(number)

    def step(t, carry):
        for number in range(len(reach)):
            if number + 1 < STEPS - 1:

                @pl.when(t == number + 1)
                def _():
                    meet(number)

        for c, (begin, rows) in enumerate(chunks):
            arrived(t, c)

            def group(g, inner):
                z = begin + g * GROUP
                field[t + 2, pl.ds(REACH + z, GROUP), own, :] = advance(t, z)
                return inner

            lax.fori_loop(0, rows // GROUP, group, 0, unroll=True)
            send(t + 1, c)
        return carry

    lax.fori_loop(0, STEPS - 1, step, 0)
    for number in range(len(reach)):
        if number + 1 >= STEPS - 1:
            meet(number)
    if reach:
        greeted(len(reach) - 1)

    def landing(who):
        return image.at[:, pl.ds(pl.multiple_of(who * width, width), width), :]

    def piece(peer):
        return pltpu.make_async_remote_copy(
            src_ref=slab.at[pl.ds(peer * slab_depth, slab_depth), :, :],
            dst_ref=landing(me),
            send_sem=img_send.at[peer],
            recv_sem=img_recv.at[me],
            device_id={"gx": peer},
            device_id_type=pl.DeviceIdType.MESH,
        )

    def filtered(peer):
        z = peer * slab_depth
        return (
            2.0 * product[pl.ds(1 + z, slab_depth), :, :]
            - product[pl.ds(z, slab_depth), :, :]
            - product[pl.ds(2 + z, slab_depth), :, :]
        )

    def ship(low, count):
        def one(j, carry):
            peer = low + lax.rem(me + 1 + j, count)
            value = filtered(peer)

            @pl.when(peer != me)
            def _():
                slab[pl.ds(peer * slab_depth, slab_depth), :, :] = value
                piece(peer).start()

            @pl.when(peer == me)
            def _():
                landing(me)[...] = value

            return carry

        lax.fori_loop(0, count, one, 0)

    local[6].wait()
    ground = rdepth_v[...]
    last = STEPS - 1
    ready, gone = set(), set()
    for c, (begin, rows) in enumerate(chunks):
        arrived(last, c)

        def group(g, inner):
            z = begin + g * GROUP
            new = advance(last, z)
            final[pl.ds(z, GROUP), :, :] = new
            levels = lax.broadcasted_iota(jnp.int32, (GROUP, width, length), 0) + z
            masked = jnp.where(levels >= ground[None], receiver_v[pl.ds(z, GROUP), :, :], 0.0)
            product[pl.ds(1 + z, GROUP), :, :] = new * masked
            return inner

        lax.fori_loop(0, rows // GROUP, group, 0, unroll=True)
        ready |= set(range(begin, begin + rows))
        able = [
            peer
            for peer in range(nx)
            if peer not in gone
            and all(
                level in ready
                for level in range(
                    max(peer * slab_depth - 1, 0), min((peer + 1) * slab_depth + 1, depth)
                )
            )
        ]
        gone |= set(able)
        low = 0
        while low < len(able):
            high = low + 1
            while high < len(able) and able[high] == able[high - 1] + 1:
                high += 1
            ship(able[low], high - low)
            low = high

    def drain(t, carry):
        for c in range(len(chunks)):
            sent(t, c)
        return carry

    lax.fori_loop(0, STEPS, drain, 0)

    def finish(j, carry):
        peer = lax.rem(me + j, nx)
        piece(peer).wait_send()
        came = lax.rem(me + nx - j, nx)
        pltpu.make_async_remote_copy(
            src_ref=slab.at[pl.ds(me * slab_depth, slab_depth), :, :],
            dst_ref=landing(came),
            send_sem=img_send.at[came],
            recv_sem=img_recv.at[came],
            device_id={"gx": came},
            device_id_type=pl.DeviceIdType.MESH,
        ).wait_recv()
        return carry

    lax.fori_loop(1, nx, finish, 0)


def solution(mesh):
    nx, ny = mesh.shape["gx"], mesh.shape["gy"]

    def shards(pressure, prior, courant, wavelet, delay, sdepth, rdepth, receiver):
        depth, width, length = pressure.shape
        parts = len(chunks_of(depth))
        hbm = pl.BlockSpec(memory_space=pl.ANY)
        vmem = pl.BlockSpec(memory_space=pltpu.VMEM)
        flat = (depth, width, length)
        sides = (STEPS, 2, depth, width, length) if ny > 1 else (1, 1, 1, width, length)
        return pl.pallas_call(
            functools.partial(kernel, nx, ny),
            out_shape=(
                pltpu.VMEM(flat, jnp.float32),
                pltpu.VMEM((depth // nx, width * nx, length), jnp.float32),
            ),
            in_specs=[hbm] * 8,
            out_specs=(vmem, vmem),
            scratch_shapes=[
                pltpu.VMEM((STEPS + 1, depth + 2 * REACH, width + 2 * REACH, length), jnp.float32),
                pltpu.VMEM(sides, jnp.float32),
                pltpu.VMEM(flat, jnp.bfloat16),
                pltpu.VMEM(flat, jnp.float32),
                pltpu.VMEM((STEPS, width, length), jnp.float32),
                pltpu.VMEM((depth + 2, width, length), jnp.float32),
                pltpu.VMEM(flat, jnp.float32),
                pltpu.VMEM((2 * length, 2 * length), jnp.bfloat16),
                pltpu.SMEM(wavelet.shape, jnp.float32),
                pltpu.VMEM((width, length), jnp.int32),
                pltpu.VMEM((width, length), jnp.int32),
                pltpu.VMEM((width, length), jnp.int32),
                pltpu.SemaphoreType.DMA((parts,)),
                pltpu.SemaphoreType.DMA((7,)),
                pltpu.SemaphoreType.DMA((STEPS, parts, 2)),
                pltpu.SemaphoreType.DMA((STEPS, parts, 2)),
                pltpu.SemaphoreType.DMA((STEPS, parts, 2)),
                pltpu.SemaphoreType.DMA((STEPS, parts, 2)),
                pltpu.SemaphoreType.DMA((nx,)),
                pltpu.SemaphoreType.DMA((nx,)),
                pltpu.SemaphoreType.REGULAR((max(nx.bit_length(), 1), 2)),
            ],
            compiler_params=pltpu.CompilerParams(
                collective_id=0, has_side_effects=True, vmem_limit_bytes=60000000
            ),
        )(pressure, prior, courant, wavelet, delay, sdepth, rdepth, receiver)

    in_specs = (
        P(None, ("shots", "gx"), "gy"),
        P(None, ("shots", "gx"), "gy"),
        P(None, "gx", "gy"),
        P("shots"),
        P(("shots", "gx"), "gy"),
        P(("shots", "gx"), "gy"),
        P(("shots", "gx"), "gy"),
        P(None, ("shots", "gx"), "gy"),
    )
    out_specs = (P(None, ("shots", "gx"), "gy"), P("gx", "shots", "gy"))
    return jax.shard_map(shards, mesh=mesh, in_specs=in_specs, out_specs=out_specs, check_vma=False)
```

```python
import functools

import jax
import jax.numpy as jnp
from jax import lax
from jax.experimental import pallas as pl
from jax.experimental.pallas import tpu as pltpu
from jax.sharding import PartitionSpec as P

STEPS = 8
REACH = 4
CENTER = -205.0 / 72.0
COEFS = (1.6, -0.2, 8.0 / 315.0, -1.0 / 560.0)
GROUP = 8


def chunks_of(depth):
    quarter = depth // 4
    return tuple((quarter * c, quarter) for c in (0, 3, 1, 2))


def kernel(
    nx,
    ny,
    pressure,
    prior,
    courant,
    wavelet,
    delay,
    sdepth,
    rdepth,
    receiver,
    final,
    image,
    field,
    side,
    courant_v,
    receiver_v,
    amp,
    product,
    slab,
    weights,
    wave_v,
    delay_v,
    sdepth_v,
    rdepth_v,
    first_sem,
    local_sem,
    send_sem,
    recv_sem,
    side_send,
    side_recv,
    img_send,
    img_recv,
    known,
):
    depth, width, length = pressure.shape
    chunks = chunks_of(depth)
    slab_depth = depth // nx
    me = lax.axis_index("gx")
    mine = lax.axis_index("gy")
    own = pl.ds(REACH, width)

    barrier = pltpu.get_barrier_semaphore()

    def toward(way, far):
        return (me + far, me + far < nx) if way == 0 else (me - far, me >= far)

    if nx > 1:
        for way in (0, 1):
            peer, there = toward(way, 1)

            @pl.when(there)
            def _():
                pl.semaphore_signal(
                    barrier,
                    inc=1,
                    device_id={"gx": peer},
                    device_id_type=pl.DeviceIdType.MESH,
                )

    for j in range(1, ny):
        pl.semaphore_signal(
            barrier,
            inc=1,
            device_id={"gy": lax.rem(mine + j, ny)},
            device_id_type=pl.DeviceIdType.MESH,
        )

    first = [
        pltpu.make_async_copy(
            pressure.at[pl.ds(z, rows), :, :],
            field.at[1, pl.ds(REACH + z, rows), own, :],
            first_sem.at[c],
        )
        for c, (z, rows) in enumerate(chunks)
    ]
    local = [
        pltpu.make_async_copy(prior, field.at[0, pl.ds(REACH, depth), own, :], local_sem.at[0]),
        pltpu.make_async_copy(courant, courant_v, local_sem.at[1]),
        pltpu.make_async_copy(wavelet, wave_v, local_sem.at[2]),
        pltpu.make_async_copy(delay, delay_v, local_sem.at[3]),
        pltpu.make_async_copy(sdepth, sdepth_v, local_sem.at[4]),
        pltpu.make_async_copy(rdepth, rdepth_v, local_sem.at[5]),
        pltpu.make_async_copy(receiver, receiver_v, local_sem.at[6]),
    ]
    def span(c):
        z, rows = chunks[c]
        return pl.ds(REACH + z, rows)

    def face(t, c, way, opening):
        z, rows = chunks[c]
        source = width - REACH if way == 0 else 0
        target = 0 if way == 0 else REACH + width
        return pltpu.make_async_remote_copy(
            src_ref=pressure.at[pl.ds(z, rows), pl.ds(source, REACH), :]
            if opening
            else field.at[t + 1, span(c), pl.ds(REACH + source, REACH), :],
            dst_ref=field.at[t + 1, span(c), pl.ds(target, REACH), :],
            send_sem=send_sem.at[t % 2, c, way],
            recv_sem=recv_sem.at[t % 2, c, way],
            device_id={"gx": lax.rem(me + (1 if way == 0 else nx - 1), nx)},
            device_id_type=pl.DeviceIdType.MESH,
        )

    def flank(t, c, way, opening):
        peer = lax.rem(mine + 1, ny) if way == 0 else lax.rem(mine + ny - 1, ny)
        z, rows = chunks[c]
        return pltpu.make_async_remote_copy(
            src_ref=pressure.at[pl.ds(z, rows), :, :]
            if opening
            else field.at[t + 1, span(c), own, :],
            dst_ref=side.at[t, way, pl.ds(z, rows), :, :],
            send_sem=side_send.at[t % 2, c, way],
            recv_sem=side_recv.at[t % 2, c, way],
            device_id={"gy": peer},
            device_id_type=pl.DeviceIdType.MESH,
        )

    def each_face(t, c, act, sending, opening=False):
        if nx > 1:
            for way in (0, 1):
                there = me < nx - 1 if (way == 0) == sending else me > 0

                @pl.when(there)
                def _():
                    act(face(t, c, way, opening))

        if ny > 1:
            for way in (0, 1):
                there = mine < ny - 1 if (way == 0) == sending else mine > 0

                @pl.when(there)
                def _():
                    act(flank(t, c, way, opening))

    def send(t, c, opening=False):
        each_face(t, c, lambda copy: copy.start(), True, opening)

    def sent(t, c):
        each_face(t, c, lambda copy: copy.wait_send(), True)

    def arrived(t, c):
        each_face(t, c, lambda copy: copy.wait_recv(), False)

    beside = (me > 0).astype(jnp.int32) + (me < nx - 1).astype(jnp.int32)
    if nx > 1 or ny > 1:
        pl.semaphore_wait(barrier, beside + ny - 1)

    for c in range(len(chunks)):
        send(0, c, opening=True)
    for copy in first + local:
        copy.start()

    rim = jnp.zeros((REACH, width + 2 * REACH, length), jnp.float32)
    for t in range(STEPS):
        field[t + 1, pl.ds(0, REACH), :, :] = rim
        field[t + 1, pl.ds(REACH + depth, REACH), :, :] = rim

    def clear(at):
        def one(t, carry):
            field[t + 1, pl.ds(REACH, depth), pl.ds(at, REACH), :] = jnp.zeros(
                (depth, REACH, length), jnp.float32
            )
            return carry

        lax.fori_loop(0, STEPS, one, 0)

    @pl.when(me == 0)
    def _():
        clear(0)

    @pl.when(me == nx - 1)
    def _():
        clear(REACH + width)

    if ny > 1:

        def clear_side(k):
            def one(t, carry):
                side[t, k] = jnp.zeros((depth, width, length), jnp.float32)
                return carry

            lax.fori_loop(0, STEPS, one, 0)

        @pl.when(mine == 0)
        def _():
            clear_side(0)

        @pl.when(mine == ny - 1)
        def _():
            clear_side(1)

    product[pl.ds(0, 1), :, :] = jnp.zeros((1, width, length), jnp.float32)
    product[pl.ds(depth + 1, 1), :, :] = jnp.zeros((1, width, length), jnp.float32)

    start = lax.broadcasted_iota(jnp.int32, (length, length), 0)
    gap = jnp.abs(start - lax.broadcasted_iota(jnp.int32, (length, length), 1))
    band = jnp.where(gap == 0, 3.0 * CENTER, 0.0)
    for k in range(1, REACH + 1):
        band = jnp.where(gap == k, COEFS[k - 1], band)
    band_high = band.astype(jnp.bfloat16)
    band_low = (band - band_high.astype(jnp.float32)).astype(jnp.bfloat16)
    weights[...] = jnp.concatenate(
        [
            jnp.concatenate([band_high, band_low], axis=1),
            jnp.concatenate([band_high, jnp.zeros_like(band_low)], axis=1),
        ],
        axis=0,
    )

    for copy in first + local[:6]:
        copy.wait()
    late = delay_v[...]
    for t in range(STEPS):
        total = jnp.zeros((width, length), jnp.float32)
        for pick in range(wavelet.shape[0]):
            total = total + jnp.where(late + t == pick, wave_v[pick], 0.0)
        amp[t] = total

    lanes = lax.broadcasted_iota(jnp.int32, (width, length), 1)
    origin = sdepth_v[...]

    def along(v):
        tall = v.reshape(GROUP * width, length)
        high = tall.astype(jnp.bfloat16)
        low = (tall - high.astype(jnp.float32)).astype(jnp.bfloat16)
        both = jnp.dot(
            jnp.concatenate([high, low], axis=1), weights[...], preferred_element_type=jnp.float32
        )
        return (both[:, :length] + both[:, length:]).reshape(GROUP, width, length)

    def advance(t, z):
        at = t + 1
        v = field[at, pl.ds(REACH + z, GROUP), own, :]
        old = field[t, pl.ds(REACH + z, GROUP), own, :]
        total = (3.0 * CENTER) * v if ny > 1 else along(v)
        for k in range(1, REACH + 1):
            near = (
                field[at, pl.ds(REACH + z + k, GROUP), own, :]
                + field[at, pl.ds(REACH + z - k, GROUP), own, :]
            )
            near = near + (
                field[at, pl.ds(REACH + z, GROUP), pl.ds(REACH + k, width), :]
                + field[at, pl.ds(REACH + z, GROUP), pl.ds(REACH - k, width), :]
            )
            total = total + COEFS[k - 1] * near
            if ny > 1:
                up = pltpu.roll(v, length - k, 2)
                down = pltpu.roll(v, k, 2)
                low = pltpu.roll(side[t, 0, pl.ds(z, GROUP), :, :], k, 2)
                high = pltpu.roll(side[t, 1, pl.ds(z, GROUP), :, :], length - k, 2)
                up = jnp.where((lanes < length - k)[None], up, high)
                down = jnp.where((lanes >= k)[None], down, low)
                total = total + COEFS[k - 1] * (up + down)
        strength = courant_v[pl.ds(z, GROUP), :, :].astype(jnp.float32)
        levels = lax.broadcasted_iota(jnp.int32, (GROUP, width, length), 0) + z
        shot = jnp.where(levels == origin[None], amp[t][None], 0.0)
        return 2.0 * v - old + strength * total + shot

    reach = []
    while (reach[-1] * 2 if reach else 1) < nx:
        reach.append(reach[-1] * 2 if reach else 1)

    def greet(number):
        for way in (0, 1):
            peer, there = toward(way, reach[number])

            @pl.when(there)
            def _():
                pl.semaphore_signal(
                    known.at[number, way],
                    inc=1,
                    device_id={"gx": peer},
                    device_id_type=pl.DeviceIdType.MESH,
                )

    def greeted(number):
        for way in (0, 1):
            there = toward(1 - way, reach[number])[1]

            @pl.when(there)
            def _():
                pl.semaphore_wait(known.at[number, way], 1)

    def meet(number):
        if number > 0:
            greeted(number - 1)
        greet(number)

    def step(t, carry):
        for number in range(len(reach)):
            if number + 1 < STEPS - 1:

                @pl.when(t == number + 1)
                def _():
                    meet(number)

        for c, (begin, rows) in enumerate(chunks):
            arrived(t, c)

            def group(g, inner):
                z = begin + g * GROUP
                field[t + 2, pl.ds(REACH + z, GROUP), own, :] = advance(t, z)
                return inner

            lax.fori_loop(0, rows // GROUP, group, 0, unroll=True)

            @pl.when(t > 0)
            def _():
                sent(t - 1, c)

            send(t + 1, c)
        return carry

    lax.fori_loop(0, STEPS - 1, step, 0)
    for number in range(len(reach)):
        if number + 1 >= STEPS - 1:
            meet(number)
    if reach:
        greeted(len(reach) - 1)

    def landing(who):
        return image.at[:, pl.ds(pl.multiple_of(who * width, width), width), :]

    def piece(peer):
        return pltpu.make_async_remote_copy(
            src_ref=slab.at[pl.ds(peer * slab_depth, slab_depth), :, :],
            dst_ref=landing(me),
            send_sem=img_send,
            recv_sem=img_recv,
            device_id={"gx": peer},
            device_id_type=pl.DeviceIdType.MESH,
        )

    def filtered(peer):
        z = peer * slab_depth
        return (
            2.0 * product[pl.ds(1 + z, slab_depth), :, :]
            - product[pl.ds(z, slab_depth), :, :]
            - product[pl.ds(2 + z, slab_depth), :, :]
        )

    def ship(low, count):
        def one(j, carry):
            peer = low + lax.rem(me + 1 + j, count)
            value = filtered(peer)

            @pl.when(peer != me)
            def _():
                slab[pl.ds(peer * slab_depth, slab_depth), :, :] = value
                piece(peer).start()

            @pl.when(peer == me)
            def _():
                landing(me)[...] = value

            return carry

        lax.fori_loop(0, count, one, 0)

    local[6].wait()
    ground = rdepth_v[...]
    last = STEPS - 1
    ready, gone = set(), set()
    for c, (begin, rows) in enumerate(chunks):
        arrived(last, c)

        def group(g, inner):
            z = begin + g * GROUP
            new = advance(last, z)
            final[pl.ds(z, GROUP), :, :] = new
            levels = lax.broadcasted_iota(jnp.int32, (GROUP, width, length), 0) + z
            masked = jnp.where(levels >= ground[None], receiver_v[pl.ds(z, GROUP), :, :], 0.0)
            product[pl.ds(1 + z, GROUP), :, :] = new * masked
            return inner

        lax.fori_loop(0, rows // GROUP, group, 0, unroll=True)
        ready |= set(range(begin, begin + rows))
        able = [
            peer
            for peer in range(nx)
            if peer not in gone
            and all(
                level in ready
                for level in range(
                    max(peer * slab_depth - 1, 0), min((peer + 1) * slab_depth + 1, depth)
                )
            )
        ]
        gone |= set(able)
        low = 0
        while low < len(able):
            high = low + 1
            while high < len(able) and able[high] == able[high - 1] + 1:
                high += 1
            ship(able[low], high - low)
            low = high

    for t in range(max(STEPS - 2, 0), STEPS):
        for c in range(len(chunks)):
            sent(t, c)
    if nx > 1:
        others = pltpu.make_async_remote_copy(
            src_ref=slab.at[pl.ds(0, (nx - 1) * slab_depth), :, :],
            dst_ref=image.at[:, pl.ds(0, (nx - 1) * width), :],
            send_sem=img_send,
            recv_sem=img_recv,
            device_id={"gx": lax.rem(me + 1, nx)},
            device_id_type=pl.DeviceIdType.MESH,
        )
        others.wait_send()
        others.wait_recv()


def solution(mesh):
    nx, ny = mesh.shape["gx"], mesh.shape["gy"]

    def shards(pressure, prior, courant, wavelet, delay, sdepth, rdepth, receiver):
        depth, width, length = pressure.shape
        parts = len(chunks_of(depth))
        hbm = pl.BlockSpec(memory_space=pl.ANY)
        vmem = pl.BlockSpec(memory_space=pltpu.VMEM)
        flat = (depth, width, length)
        sides = (STEPS, 2, depth, width, length) if ny > 1 else (1, 1, 1, width, length)
        return pl.pallas_call(
            functools.partial(kernel, nx, ny),
            out_shape=(
                pltpu.VMEM(flat, jnp.float32),
                pltpu.VMEM((depth // nx, width * nx, length), jnp.float32),
            ),
            in_specs=[hbm] * 8,
            out_specs=(vmem, vmem),
            scratch_shapes=[
                pltpu.VMEM((STEPS + 1, depth + 2 * REACH, width + 2 * REACH, length), jnp.float32),
                pltpu.VMEM(sides, jnp.float32),
                pltpu.VMEM(flat, jnp.bfloat16),
                pltpu.VMEM(flat, jnp.float32),
                pltpu.VMEM((STEPS, width, length), jnp.float32),
                pltpu.VMEM((depth + 2, width, length), jnp.float32),
                pltpu.VMEM(flat, jnp.float32),
                pltpu.VMEM((2 * length, 2 * length), jnp.bfloat16),
                pltpu.SMEM(wavelet.shape, jnp.float32),
                pltpu.VMEM((width, length), jnp.int32),
                pltpu.VMEM((width, length), jnp.int32),
                pltpu.VMEM((width, length), jnp.int32),
                pltpu.SemaphoreType.DMA((parts,)),
                pltpu.SemaphoreType.DMA((7,)),
                pltpu.SemaphoreType.DMA((2, parts, 2)),
                pltpu.SemaphoreType.DMA((2, parts, 2)),
                pltpu.SemaphoreType.DMA((2, parts, 2) if ny > 1 else (1, 1, 1)),
                pltpu.SemaphoreType.DMA((2, parts, 2) if ny > 1 else (1, 1, 1)),
                pltpu.SemaphoreType.DMA,
                pltpu.SemaphoreType.DMA,
                pltpu.SemaphoreType.REGULAR((max((nx - 1).bit_length(), 1), 2)),
            ],
            compiler_params=pltpu.CompilerParams(
                collective_id=0, has_side_effects=True, vmem_limit_bytes=60000000
            ),
        )(pressure, prior, courant, wavelet, delay, sdepth, rdepth, receiver)

    in_specs = (
        P(None, ("shots", "gx"), "gy"),
        P(None, ("shots", "gx"), "gy"),
        P(None, "gx", "gy"),
        P("shots"),
        P(("shots", "gx"), "gy"),
        P(("shots", "gx"), "gy"),
        P(("shots", "gx"), "gy"),
        P(None, ("shots", "gx"), "gy"),
    )
    out_specs = (P(None, ("shots", "gx"), "gy"), P("gx", "shots", "gy"))
    return jax.shard_map(shards, mesh=mesh, in_specs=in_specs, out_specs=out_specs, check_vma=False)
```

```python
import functools

import jax
import jax.numpy as jnp
from jax import lax
from jax.experimental import pallas as pl
from jax.experimental.pallas import tpu as pltpu
from jax.sharding import PartitionSpec as P

STEPS = 8
REACH = 4
CENTER = -205.0 / 72.0
COEFS = (1.6, -0.2, 8.0 / 315.0, -1.0 / 560.0)
GROUP = 8


def chunks_of(depth):
    quarter = depth // 4
    return tuple((quarter * c, quarter) for c in (0, 3, 1, 2))


def kernel(
    nx,
    ny,
    pressure,
    prior,
    courant,
    wavelet,
    delay,
    sdepth,
    rdepth,
    receiver,
    final,
    image,
    field,
    side,
    courant_v,
    receiver_v,
    amp,
    product,
    slab,
    weights,
    wave_v,
    delay_v,
    sdepth_v,
    rdepth_v,
    local_sem,
    send_sem,
    recv_sem,
    side_send,
    side_recv,
    img_send,
    img_recv,
    known,
):
    depth, width, length = pressure.shape
    chunks = chunks_of(depth)
    slab_depth = depth // nx
    me = lax.axis_index("gx")
    mine = lax.axis_index("gy")
    own = pl.ds(REACH, width)

    barrier = pltpu.get_barrier_semaphore()

    def toward(way, far):
        return (me + far, me + far < nx) if way == 0 else (me - far, me >= far)

    if nx > 1:
        for way in (0, 1):
            peer, there = toward(way, 1)

            @pl.when(there)
            def _():
                pl.semaphore_signal(
                    barrier,
                    inc=1,
                    device_id={"gx": peer},
                    device_id_type=pl.DeviceIdType.MESH,
                )

    for j in range(1, ny):
        pl.semaphore_signal(
            barrier,
            inc=1,
            device_id={"gy": lax.rem(mine + j, ny)},
            device_id_type=pl.DeviceIdType.MESH,
        )

    local = [
        pltpu.make_async_copy(prior, field.at[0, pl.ds(REACH, depth), own, :], local_sem.at[0]),
        pltpu.make_async_copy(courant, courant_v, local_sem.at[1]),
        pltpu.make_async_copy(wavelet, wave_v, local_sem.at[2]),
        pltpu.make_async_copy(delay, delay_v, local_sem.at[3]),
        pltpu.make_async_copy(sdepth, sdepth_v, local_sem.at[4]),
        pltpu.make_async_copy(rdepth, rdepth_v, local_sem.at[5]),
        pltpu.make_async_copy(receiver, receiver_v, local_sem.at[6]),
        pltpu.make_async_copy(pressure, field.at[1, pl.ds(REACH, depth), own, :], local_sem.at[7]),
    ]
    def span(c):
        z, rows = chunks[c]
        return pl.ds(REACH + z, rows)

    def face(t, c, way, opening):
        z, rows = chunks[c]
        source = width - REACH if way == 0 else 0
        target = 0 if way == 0 else REACH + width
        return pltpu.make_async_remote_copy(
            src_ref=pressure.at[pl.ds(z, rows), pl.ds(source, REACH), :]
            if opening
            else field.at[t + 1, span(c), pl.ds(REACH + source, REACH), :],
            dst_ref=field.at[t + 1, span(c), pl.ds(target, REACH), :],
            send_sem=send_sem.at[t % 2, c, way],
            recv_sem=recv_sem.at[t % 2, c, way],
            device_id={"gx": lax.rem(me + (1 if way == 0 else nx - 1), nx)},
            device_id_type=pl.DeviceIdType.MESH,
        )

    def flank(t, c, way, opening):
        peer = lax.rem(mine + 1, ny) if way == 0 else lax.rem(mine + ny - 1, ny)
        z, rows = chunks[c]
        return pltpu.make_async_remote_copy(
            src_ref=pressure.at[pl.ds(z, rows), :, :]
            if opening
            else field.at[t + 1, span(c), own, :],
            dst_ref=side.at[t, way, pl.ds(z, rows), :, :],
            send_sem=side_send.at[t % 2, c, way],
            recv_sem=side_recv.at[t % 2, c, way],
            device_id={"gy": peer},
            device_id_type=pl.DeviceIdType.MESH,
        )

    def each_face(t, c, act, sending, opening=False):
        if nx > 1:
            for way in (0, 1):
                there = me < nx - 1 if (way == 0) == sending else me > 0

                @pl.when(there)
                def _():
                    act(face(t, c, way, opening))

        if ny > 1:
            for way in (0, 1):
                there = mine < ny - 1 if (way == 0) == sending else mine > 0

                @pl.when(there)
                def _():
                    act(flank(t, c, way, opening))

    def send(t, c, opening=False):
        each_face(t, c, lambda copy: copy.start(), True, opening)

    def sent(t, c):
        each_face(t, c, lambda copy: copy.wait_send(), True)

    def arrived(t, c):
        each_face(t, c, lambda copy: copy.wait_recv(), False)

    beside = (me > 0).astype(jnp.int32) + (me < nx - 1).astype(jnp.int32)
    if nx > 1 or ny > 1:
        pl.semaphore_wait(barrier, beside + ny - 1)

    for c in range(len(chunks)):
        send(0, c, opening=True)
    for copy in local[::-1]:
        copy.start()

    rim = jnp.zeros((REACH, width + 2 * REACH, length), jnp.float32)
    for t in range(STEPS):
        field[t + 1, pl.ds(0, REACH), :, :] = rim
        field[t + 1, pl.ds(REACH + depth, REACH), :, :] = rim

    def clear(at):
        def one(t, carry):
            field[t + 1, pl.ds(REACH, depth), pl.ds(at, REACH), :] = jnp.zeros(
                (depth, REACH, length), jnp.float32
            )
            return carry

        lax.fori_loop(0, STEPS, one, 0)

    @pl.when(me == 0)
    def _():
        clear(0)

    @pl.when(me == nx - 1)
    def _():
        clear(REACH + width)

    if ny > 1:

        def clear_side(k):
            def one(t, carry):
                side[t, k] = jnp.zeros((depth, width, length), jnp.float32)
                return carry

            lax.fori_loop(0, STEPS, one, 0)

        @pl.when(mine == 0)
        def _():
            clear_side(0)

        @pl.when(mine == ny - 1)
        def _():
            clear_side(1)

    product[pl.ds(0, 1), :, :] = jnp.zeros((1, width, length), jnp.float32)
    product[pl.ds(depth + 1, 1), :, :] = jnp.zeros((1, width, length), jnp.float32)

    start = lax.broadcasted_iota(jnp.int32, (length, length), 0)
    gap = jnp.abs(start - lax.broadcasted_iota(jnp.int32, (length, length), 1))
    band = jnp.where(gap == 0, 3.0 * CENTER, 0.0)
    for k in range(1, REACH + 1):
        band = jnp.where(gap == k, COEFS[k - 1], band)
    band_high = band.astype(jnp.bfloat16)
    band_low = (band - band_high.astype(jnp.float32)).astype(jnp.bfloat16)
    weights[...] = jnp.concatenate(
        [
            jnp.concatenate([band_high, band_low], axis=1),
            jnp.concatenate([band_high, jnp.zeros_like(band_low)], axis=1),
        ],
        axis=0,
    )

    for copy in local[:6] + local[7:]:
        copy.wait()
    late = delay_v[...]
    for t in range(STEPS):
        total = jnp.zeros((width, length), jnp.float32)
        for pick in range(wavelet.shape[0]):
            total = total + jnp.where(late + t == pick, wave_v[pick], 0.0)
        amp[t] = total

    lanes = lax.broadcasted_iota(jnp.int32, (width, length), 1)
    origin = sdepth_v[...]

    def along(v):
        tall = v.reshape(GROUP * width, length)
        high = tall.astype(jnp.bfloat16)
        low = (tall - high.astype(jnp.float32)).astype(jnp.bfloat16)
        both = jnp.dot(
            jnp.concatenate([high, low], axis=1), weights[...], preferred_element_type=jnp.float32
        )
        return (both[:, :length] + both[:, length:]).reshape(GROUP, width, length)

    def advance(t, z):
        at = t + 1
        v = field[at, pl.ds(REACH + z, GROUP), own, :]
        old = field[t, pl.ds(REACH + z, GROUP), own, :]
        total = (3.0 * CENTER) * v if ny > 1 else along(v)
        for k in range(1, REACH + 1):
            near = (
                field[at, pl.ds(REACH + z + k, GROUP), own, :]
                + field[at, pl.ds(REACH + z - k, GROUP), own, :]
            )
            near = near + (
                field[at, pl.ds(REACH + z, GROUP), pl.ds(REACH + k, width), :]
                + field[at, pl.ds(REACH + z, GROUP), pl.ds(REACH - k, width), :]
            )
            total = total + COEFS[k - 1] * near
            if ny > 1:
                up = pltpu.roll(v, length - k, 2)
                down = pltpu.roll(v, k, 2)
                low = pltpu.roll(side[t, 0, pl.ds(z, GROUP), :, :], k, 2)
                high = pltpu.roll(side[t, 1, pl.ds(z, GROUP), :, :], length - k, 2)
                up = jnp.where((lanes < length - k)[None], up, high)
                down = jnp.where((lanes >= k)[None], down, low)
                total = total + COEFS[k - 1] * (up + down)
        strength = courant_v[pl.ds(z, GROUP), :, :].astype(jnp.float32)
        levels = lax.broadcasted_iota(jnp.int32, (GROUP, width, length), 0) + z
        shot = jnp.where(levels == origin[None], amp[t][None], 0.0)
        return 2.0 * v - old + strength * total + shot

    reach = []
    while (reach[-1] * 2 if reach else 1) < nx:
        reach.append(reach[-1] * 2 if reach else 1)

    def greet(number):
        for way in (0, 1):
            peer, there = toward(way, reach[number])

            @pl.when(there)
            def _():
                pl.semaphore_signal(
                    known.at[number, way],
                    inc=1,
                    device_id={"gx": peer},
                    device_id_type=pl.DeviceIdType.MESH,
                )

    def greeted(number):
        for way in (0, 1):
            there = toward(1 - way, reach[number])[1]

            @pl.when(there)
            def _():
                pl.semaphore_wait(known.at[number, way], 1)

    def meet(number):
        if number > 0:
            greeted(number - 1)
        greet(number)

    def step(t, carry):
        for number in range(len(reach)):
            if number + 1 < STEPS - 1:

                @pl.when(t == number + 1)
                def _():
                    meet(number)

        for c, (begin, rows) in enumerate(chunks):
            arrived(t, c)

            @pl.when(t > 0)
            def _():
                sent(t - 1, c)

            def group(g, inner):
                z = begin + g * GROUP
                field[t + 2, pl.ds(REACH + z, GROUP), own, :] = advance(t, z)
                return inner

            lax.fori_loop(0, rows // GROUP, group, 0, unroll=True)
            send(t + 1, c)
        return carry

    lax.fori_loop(0, STEPS - 1, step, 0)
    for number in range(len(reach)):
        if number + 1 >= STEPS - 1:
            meet(number)
    if reach:
        greeted(len(reach) - 1)

    def landing(who):
        return image.at[:, pl.ds(pl.multiple_of(who * width, width), width), :]

    def piece(peer):
        return pltpu.make_async_remote_copy(
            src_ref=slab.at[pl.ds(peer * slab_depth, slab_depth), :, :],
            dst_ref=landing(me),
            send_sem=img_send,
            recv_sem=img_recv,
            device_id={"gx": peer},
            device_id_type=pl.DeviceIdType.MESH,
        )

    def filtered(peer):
        z = peer * slab_depth
        return (
            2.0 * product[pl.ds(1 + z, slab_depth), :, :]
            - product[pl.ds(z, slab_depth), :, :]
            - product[pl.ds(2 + z, slab_depth), :, :]
        )

    def ship(low, count):
        def one(j, carry):
            peer = low + lax.rem(me + 1 + j, count)
            value = filtered(peer)

            @pl.when(peer != me)
            def _():
                slab[pl.ds(peer * slab_depth, slab_depth), :, :] = value
                piece(peer).start()

            @pl.when(peer == me)
            def _():
                landing(me)[...] = value

            return carry

        lax.fori_loop(0, count, one, 0)

    local[6].wait()
    ground = rdepth_v[...]
    last = STEPS - 1
    ready, gone = set(), set()
    for c, (begin, rows) in enumerate(chunks):
        arrived(last, c)

        def group(g, inner):
            z = begin + g * GROUP
            new = advance(last, z)
            final[pl.ds(z, GROUP), :, :] = new
            levels = lax.broadcasted_iota(jnp.int32, (GROUP, width, length), 0) + z
            masked = jnp.where(levels >= ground[None], receiver_v[pl.ds(z, GROUP), :, :], 0.0)
            product[pl.ds(1 + z, GROUP), :, :] = new * masked
            return inner

        lax.fori_loop(0, rows // GROUP, group, 0, unroll=True)
        ready |= set(range(begin, begin + rows))
        able = [
            peer
            for peer in range(nx)
            if peer not in gone
            and all(
                level in ready
                for level in range(
                    max(peer * slab_depth - 1, 0), min((peer + 1) * slab_depth + 1, depth)
                )
            )
        ]
        gone |= set(able)
        low = 0
        while low < len(able):
            high = low + 1
            while high < len(able) and able[high] == able[high - 1] + 1:
                high += 1
            ship(able[low], high - low)
            low = high

    for t in range(max(STEPS - 2, 0), STEPS):
        for c in range(len(chunks)):
            sent(t, c)
    if nx > 1:
        others = pltpu.make_async_remote_copy(
            src_ref=slab.at[pl.ds(0, (nx - 1) * slab_depth), :, :],
            dst_ref=image.at[:, pl.ds(0, (nx - 1) * width), :],
            send_sem=img_send,
            recv_sem=img_recv,
            device_id={"gx": lax.rem(me + 1, nx)},
            device_id_type=pl.DeviceIdType.MESH,
        )
        others.wait_send()
        others.wait_recv()


def store(final_v, image_v, final, image, sem):
    copies = (
        pltpu.make_async_copy(final_v, final, sem.at[0]),
        pltpu.make_async_copy(image_v, image, sem.at[1]),
    )
    for copy in copies:
        copy.start()
    for copy in copies:
        copy.wait()


def solution(mesh):
    nx, ny = mesh.shape["gx"], mesh.shape["gy"]

    def shards(pressure, prior, courant, wavelet, delay, sdepth, rdepth, receiver):
        depth, width, length = pressure.shape
        parts = len(chunks_of(depth))
        hbm = pl.BlockSpec(memory_space=pl.ANY)
        vmem = pl.BlockSpec(memory_space=pltpu.VMEM)
        flat = (depth, width, length)
        sides = (STEPS, 2, depth, width, length) if ny > 1 else (1, 1, 1, width, length)
        deep = (depth // nx, width * nx, length)
        held = pl.pallas_call(
            functools.partial(kernel, nx, ny),
            out_shape=(
                pltpu.VMEM(flat, jnp.float32),
                pltpu.VMEM(deep, jnp.float32),
            ),
            in_specs=[hbm] * 8,
            out_specs=(vmem, vmem),
            scratch_shapes=[
                pltpu.VMEM((STEPS + 1, depth + 2 * REACH, width + 2 * REACH, length), jnp.float32),
                pltpu.VMEM(sides, jnp.float32),
                pltpu.VMEM(flat, jnp.bfloat16),
                pltpu.VMEM(flat, jnp.float32),
                pltpu.VMEM((STEPS, width, length), jnp.float32),
                pltpu.VMEM((depth + 2, width, length), jnp.float32),
                pltpu.VMEM(flat, jnp.float32),
                pltpu.VMEM((2 * length, 2 * length), jnp.bfloat16),
                pltpu.SMEM(wavelet.shape, jnp.float32),
                pltpu.VMEM((width, length), jnp.int32),
                pltpu.VMEM((width, length), jnp.int32),
                pltpu.VMEM((width, length), jnp.int32),
                pltpu.SemaphoreType.DMA((8,)),
                pltpu.SemaphoreType.DMA((2, parts, 2)),
                pltpu.SemaphoreType.DMA((2, parts, 2)),
                pltpu.SemaphoreType.DMA((2, parts, 2) if ny > 1 else (1, 1, 1)),
                pltpu.SemaphoreType.DMA((2, parts, 2) if ny > 1 else (1, 1, 1)),
                pltpu.SemaphoreType.DMA,
                pltpu.SemaphoreType.DMA,
                pltpu.SemaphoreType.REGULAR((max((nx - 1).bit_length(), 1), 2)),
            ],
            compiler_params=pltpu.CompilerParams(
                collective_id=0, has_side_effects=True, vmem_limit_bytes=60000000
            ),
        )(pressure, prior, courant, wavelet, delay, sdepth, rdepth, receiver)
        return pl.pallas_call(
            store,
            out_shape=(
                jax.ShapeDtypeStruct(flat, jnp.float32),
                jax.ShapeDtypeStruct(deep, jnp.float32),
            ),
            in_specs=[vmem] * 2,
            out_specs=(hbm, hbm),
            scratch_shapes=[pltpu.SemaphoreType.DMA((2,))],
            compiler_params=pltpu.CompilerParams(vmem_limit_bytes=4 << 20),
        )(*(pltpu.with_memory_space_constraint(part, pltpu.VMEM) for part in held))

    in_specs = (
        P(None, ("shots", "gx"), "gy"),
        P(None, ("shots", "gx"), "gy"),
        P(None, "gx", "gy"),
        P("shots"),
        P(("shots", "gx"), "gy"),
        P(("shots", "gx"), "gy"),
        P(("shots", "gx"), "gy"),
        P(None, ("shots", "gx"), "gy"),
    )
    out_specs = (P(None, ("shots", "gx"), "gy"), P("gx", "shots", "gy"))
    return jax.shard_map(shards, mesh=mesh, in_specs=in_specs, out_specs=out_specs, check_vma=False)
```

```python
import functools

import jax
import jax.numpy as jnp
from jax import lax
from jax.experimental import pallas as pl
from jax.experimental.pallas import tpu as pltpu
from jax.sharding import PartitionSpec as P

STEPS = 8
REACH = 4
CENTER = -205.0 / 72.0
COEFS = (1.6, -0.2, 8.0 / 315.0, -1.0 / 560.0)
GROUP = 8


def chunks_of(depth):
    quarter = depth // 4
    return tuple((quarter * c, quarter) for c in (0, 3, 1, 2))


def kernel(
    nx,
    ny,
    pressure,
    prior,
    courant,
    wavelet,
    delay,
    sdepth,
    rdepth,
    receiver,
    final,
    image,
    field,
    side,
    courant_v,
    receiver_v,
    partial,
    amp,
    product,
    slab,
    weights,
    wave_v,
    delay_v,
    sdepth_v,
    rdepth_v,
    local_sem,
    send_sem,
    recv_sem,
    side_send,
    side_recv,
    img_send,
    img_recv,
    known,
):
    depth, width, length = pressure.shape
    chunks = chunks_of(depth)
    slab_depth = depth // nx
    me = lax.axis_index("gx")
    mine = lax.axis_index("gy")
    own = pl.ds(REACH, width)

    barrier = pltpu.get_barrier_semaphore()

    def toward(way, far):
        return (me + far, me + far < nx) if way == 0 else (me - far, me >= far)

    if nx > 1:
        for way in (0, 1):
            peer, there = toward(way, 1)

            @pl.when(there)
            def _():
                pl.semaphore_signal(
                    barrier,
                    inc=1,
                    device_id={"gx": peer},
                    device_id_type=pl.DeviceIdType.MESH,
                )

    for j in range(1, ny):
        pl.semaphore_signal(
            barrier,
            inc=1,
            device_id={"gy": lax.rem(mine + j, ny)},
            device_id_type=pl.DeviceIdType.MESH,
        )

    local = [
        pltpu.make_async_copy(prior, field.at[0, pl.ds(REACH, depth), own, :], local_sem.at[0]),
        pltpu.make_async_copy(courant, courant_v, local_sem.at[1]),
        pltpu.make_async_copy(wavelet, wave_v, local_sem.at[2]),
        pltpu.make_async_copy(delay, delay_v, local_sem.at[3]),
        pltpu.make_async_copy(sdepth, sdepth_v, local_sem.at[4]),
        pltpu.make_async_copy(rdepth, rdepth_v, local_sem.at[5]),
        pltpu.make_async_copy(receiver, receiver_v, local_sem.at[6]),
        pltpu.make_async_copy(pressure, field.at[1, pl.ds(REACH, depth), own, :], local_sem.at[7]),
    ]
    def span(c):
        z, rows = chunks[c]
        return pl.ds(REACH + z, rows)

    def face(t, c, way, opening):
        z, rows = chunks[c]
        source = width - REACH if way == 0 else 0
        target = 0 if way == 0 else REACH + width
        return pltpu.make_async_remote_copy(
            src_ref=pressure.at[pl.ds(z, rows), pl.ds(source, REACH), :]
            if opening
            else field.at[t + 1, span(c), pl.ds(REACH + source, REACH), :],
            dst_ref=field.at[t + 1, span(c), pl.ds(target, REACH), :],
            send_sem=send_sem.at[t % 2],
            recv_sem=recv_sem.at[t % 2, c],
            device_id={"gx": lax.rem(me + (1 if way == 0 else nx - 1), nx)},
            device_id_type=pl.DeviceIdType.MESH,
        )

    def flank(t, c, way, opening):
        peer = lax.rem(mine + 1, ny) if way == 0 else lax.rem(mine + ny - 1, ny)
        z, rows = chunks[c]
        return pltpu.make_async_remote_copy(
            src_ref=pressure.at[pl.ds(z, rows), :, :]
            if opening
            else field.at[t + 1, span(c), own, :],
            dst_ref=side.at[t, way, pl.ds(z, rows), :, :],
            send_sem=side_send.at[t % 2, c, way],
            recv_sem=side_recv.at[t % 2, c, way],
            device_id={"gy": peer},
            device_id_type=pl.DeviceIdType.MESH,
        )

    def send(t, c, opening=False):
        if nx > 1:
            for way in (0, 1):

                @pl.when(me < nx - 1 if way == 0 else me > 0)
                def _():
                    face(t, c, way, opening).start()

        if ny > 1:
            for way in (0, 1):

                @pl.when(mine < ny - 1 if way == 0 else mine > 0)
                def _():
                    flank(t, c, way, opening).start()

    def faces(t, begin, rows, ways, c):
        both = field.at[t + 1, pl.ds(REACH + begin, rows), pl.ds(0, ways * REACH), :]
        return pltpu.make_async_remote_copy(
            src_ref=both,
            dst_ref=both,
            send_sem=send_sem.at[t % 2],
            recv_sem=recv_sem.at[t % 2, c],
            device_id={"gx": lax.rem(me + 1, nx)},
            device_id_type=pl.DeviceIdType.MESH,
        )

    edge = jnp.logical_or(me == 0, me == nx - 1)

    def each_count(act):
        if nx > 1:

            @pl.when(edge)
            def _():
                act(1)

        if nx > 2:

            @pl.when(jnp.logical_not(edge))
            def _():
                act(2)

    def sent(t):
        each_count(lambda ways: faces(t, 0, depth, ways, 0).wait_send())
        if ny > 1:
            for way in (0, 1):

                @pl.when(mine < ny - 1 if way == 0 else mine > 0)
                def _():
                    for c in range(len(chunks)):
                        flank(t, c, way, False).wait_send()

    def arrived(t, c):
        begin, rows = chunks[c]
        each_count(lambda ways: faces(t, begin, rows, ways, c).wait_recv())
        if ny > 1:
            for way in (0, 1):

                @pl.when(mine > 0 if way == 0 else mine < ny - 1)
                def _():
                    flank(t, c, way, False).wait_recv()

    beside = (me > 0).astype(jnp.int32) + (me < nx - 1).astype(jnp.int32)
    if nx > 1 or ny > 1:
        pl.semaphore_wait(barrier, beside + ny - 1)

    for c in range(len(chunks)):
        send(0, c, opening=True)
    for copy in local[::-1]:
        copy.start()

    rim = jnp.zeros((REACH, width + 2 * REACH, length), jnp.float32)
    for t in range(STEPS):
        field[t + 1, pl.ds(0, REACH), :, :] = rim
        field[t + 1, pl.ds(REACH + depth, REACH), :, :] = rim

    def clear(at):
        def one(t, carry):
            field[t + 1, pl.ds(REACH, depth), pl.ds(at, REACH), :] = jnp.zeros(
                (depth, REACH, length), jnp.float32
            )
            return carry

        lax.fori_loop(0, STEPS, one, 0)

    @pl.when(me == 0)
    def _():
        clear(0)

    @pl.when(me == nx - 1)
    def _():
        clear(REACH + width)

    if ny > 1:

        def clear_side(k):
            def one(t, carry):
                side[t, k] = jnp.zeros((depth, width, length), jnp.float32)
                return carry

            lax.fori_loop(0, STEPS, one, 0)

        @pl.when(mine == 0)
        def _():
            clear_side(0)

        @pl.when(mine == ny - 1)
        def _():
            clear_side(1)

    product[pl.ds(0, 1), :, :] = jnp.zeros((1, width, length), jnp.float32)
    product[pl.ds(depth + 1, 1), :, :] = jnp.zeros((1, width, length), jnp.float32)

    start = lax.broadcasted_iota(jnp.int32, (length, length), 0)
    gap = jnp.abs(start - lax.broadcasted_iota(jnp.int32, (length, length), 1))
    band = jnp.where(gap == 0, 3.0 * CENTER, 0.0)
    for k in range(1, REACH + 1):
        band = jnp.where(gap == k, COEFS[k - 1], band)
    band_high = band.astype(jnp.bfloat16)
    band_low = (band - band_high.astype(jnp.float32)).astype(jnp.bfloat16)
    weights[...] = jnp.concatenate(
        [
            jnp.concatenate([band_high, band_low], axis=1),
            jnp.concatenate([band_high, jnp.zeros_like(band_low)], axis=1),
        ],
        axis=0,
    )

    for copy in local[:6] + local[7:]:
        copy.wait()
    late = delay_v[...]
    for t in range(STEPS):
        total = jnp.zeros((width, length), jnp.float32)
        for pick in range(wavelet.shape[0]):
            total = total + jnp.where(late + t == pick, wave_v[pick], 0.0)
        amp[t] = total

    lanes = lax.broadcasted_iota(jnp.int32, (width, length), 1)
    origin = sdepth_v[...]

    def along(v):
        tall = v.reshape(GROUP * width, length)
        high = tall.astype(jnp.bfloat16)
        low = (tall - high.astype(jnp.float32)).astype(jnp.bfloat16)
        both = jnp.dot(
            jnp.concatenate([high, low], axis=1), weights[...], preferred_element_type=jnp.float32
        )
        return (both[:, :length] + both[:, length:]).reshape(GROUP, width, length)

    def prepare(t, z):
        at = t + 1
        v = field[at, pl.ds(REACH + z, GROUP), own, :]
        old = field[t, pl.ds(REACH + z, GROUP), own, :]
        total = (3.0 * CENTER) * v if ny > 1 else along(v)
        for k in range(1, REACH + 1):
            total = total + COEFS[k - 1] * (
                field[at, pl.ds(REACH + z + k, GROUP), own, :]
                + field[at, pl.ds(REACH + z - k, GROUP), own, :]
            )
        strength = courant_v[pl.ds(z, GROUP), :, :].astype(jnp.float32)
        levels = lax.broadcasted_iota(jnp.int32, (GROUP, width, length), 0) + z
        shot = jnp.where(levels == origin[None], amp[t][None], 0.0)
        partial[pl.ds(z, GROUP), :, :] = 2.0 * v - old + strength * total + shot

    def complete(t, z):
        at = t + 1
        total = None
        for k in range(1, REACH + 1):
            near = (
                field[at, pl.ds(REACH + z, GROUP), pl.ds(REACH + k, width), :]
                + field[at, pl.ds(REACH + z, GROUP), pl.ds(REACH - k, width), :]
            )
            if ny > 1:
                v = field[at, pl.ds(REACH + z, GROUP), own, :]
                up = pltpu.roll(v, length - k, 2)
                down = pltpu.roll(v, k, 2)
                low = pltpu.roll(side[t, 0, pl.ds(z, GROUP), :, :], k, 2)
                high = pltpu.roll(side[t, 1, pl.ds(z, GROUP), :, :], length - k, 2)
                up = jnp.where((lanes < length - k)[None], up, high)
                down = jnp.where((lanes >= k)[None], down, low)
                near = near + (up + down)
            total = COEFS[k - 1] * near if k == 1 else total + COEFS[k - 1] * near
        strength = courant_v[pl.ds(z, GROUP), :, :].astype(jnp.float32)
        return partial[pl.ds(z, GROUP), :, :] + strength * total

    def prepared(t, begin, rows):
        def group(g, inner):
            prepare(t, begin + g * GROUP)
            return inner

        lax.fori_loop(0, rows // GROUP, group, 0, unroll=True)

    reach = []
    while (reach[-1] * 2 if reach else 1) < nx:
        reach.append(reach[-1] * 2 if reach else 1)

    def greet(number):
        for way in (0, 1):
            peer, there = toward(way, reach[number])

            @pl.when(there)
            def _():
                pl.semaphore_signal(
                    known.at[number, way],
                    inc=1,
                    device_id={"gx": peer},
                    device_id_type=pl.DeviceIdType.MESH,
                )

    def greeted(number):
        for way in (0, 1):
            there = toward(1 - way, reach[number])[1]

            @pl.when(there)
            def _():
                pl.semaphore_wait(known.at[number, way], 1)

    def meet(number):
        if number > 0:
            greeted(number - 1)
        greet(number)

    def step(t, carry):
        for number in range(len(reach)):
            if number + 1 < STEPS - 1:

                @pl.when(t == number + 1)
                def _():
                    meet(number)

        @pl.when(t > 0)
        def _():
            sent(t - 1)

        for c, (begin, rows) in enumerate(chunks):
            prepared(t, begin, rows)
            arrived(t, c)

            def group(g, inner):
                z = begin + g * GROUP
                field[t + 2, pl.ds(REACH + z, GROUP), own, :] = complete(t, z)
                return inner

            lax.fori_loop(0, rows // GROUP, group, 0, unroll=True)
            send(t + 1, c)
        return carry

    lax.fori_loop(0, STEPS - 1, step, 0)
    for number in range(len(reach)):
        if number + 1 >= STEPS - 1:
            meet(number)
    if reach:
        greeted(len(reach) - 1)

    def landing(who):
        return image.at[:, pl.ds(pl.multiple_of(who * width, width), width), :]

    def piece(peer):
        return pltpu.make_async_remote_copy(
            src_ref=slab.at[pl.ds(peer * slab_depth, slab_depth), :, :],
            dst_ref=landing(me),
            send_sem=img_send,
            recv_sem=img_recv,
            device_id={"gx": peer},
            device_id_type=pl.DeviceIdType.MESH,
        )

    def filtered(peer):
        z = peer * slab_depth
        return (
            2.0 * product[pl.ds(1 + z, slab_depth), :, :]
            - product[pl.ds(z, slab_depth), :, :]
            - product[pl.ds(2 + z, slab_depth), :, :]
        )

    def ship(low, count):
        def one(j, carry):
            peer = low + lax.rem(me + 1 + j, count)
            value = filtered(peer)

            @pl.when(peer != me)
            def _():
                slab[pl.ds(peer * slab_depth, slab_depth), :, :] = value
                piece(peer).start()

            @pl.when(peer == me)
            def _():
                landing(me)[...] = value

            return carry

        lax.fori_loop(0, count, one, 0)

    local[6].wait()
    ground = rdepth_v[...]
    last = STEPS - 1
    ready, gone = set(), set()
    for c, (begin, rows) in enumerate(chunks):
        prepared(last, begin, rows)
        arrived(last, c)

        def group(g, inner):
            z = begin + g * GROUP
            new = complete(last, z)
            final[pl.ds(z, GROUP), :, :] = new
            levels = lax.broadcasted_iota(jnp.int32, (GROUP, width, length), 0) + z
            masked = jnp.where(levels >= ground[None], receiver_v[pl.ds(z, GROUP), :, :], 0.0)
            product[pl.ds(1 + z, GROUP), :, :] = new * masked
            return inner

        lax.fori_loop(0, rows // GROUP, group, 0, unroll=True)
        ready |= set(range(begin, begin + rows))
        able = [
            peer
            for peer in range(nx)
            if peer not in gone
            and all(
                level in ready
                for level in range(
                    max(peer * slab_depth - 1, 0), min((peer + 1) * slab_depth + 1, depth)
                )
            )
        ]
        gone |= set(able)
        low = 0
        while low < len(able):
            high = low + 1
            while high < len(able) and able[high] == able[high - 1] + 1:
                high += 1
            ship(able[low], high - low)
            low = high

    for t in range(max(STEPS - 2, 0), STEPS):
        sent(t)
    if nx > 1:
        others = pltpu.make_async_remote_copy(
            src_ref=slab.at[pl.ds(0, (nx - 1) * slab_depth), :, :],
            dst_ref=image.at[:, pl.ds(0, (nx - 1) * width), :],
            send_sem=img_send,
            recv_sem=img_recv,
            device_id={"gx": lax.rem(me + 1, nx)},
            device_id_type=pl.DeviceIdType.MESH,
        )
        others.wait_send()
        others.wait_recv()


def store(final_v, image_v, final, image, sem):
    copies = (
        pltpu.make_async_copy(final_v, final, sem.at[0]),
        pltpu.make_async_copy(image_v, image, sem.at[1]),
    )
    for copy in copies:
        copy.start()
    for copy in copies:
        copy.wait()


def solution(mesh):
    nx, ny = mesh.shape["gx"], mesh.shape["gy"]

    def shards(pressure, prior, courant, wavelet, delay, sdepth, rdepth, receiver):
        depth, width, length = pressure.shape
        parts = len(chunks_of(depth))
        hbm = pl.BlockSpec(memory_space=pl.ANY)
        vmem = pl.BlockSpec(memory_space=pltpu.VMEM)
        flat = (depth, width, length)
        sides = (STEPS, 2, depth, width, length) if ny > 1 else (1, 1, 1, width, length)
        deep = (depth // nx, width * nx, length)
        held = pl.pallas_call(
            functools.partial(kernel, nx, ny),
            out_shape=(
                pltpu.VMEM(flat, jnp.float32),
                pltpu.VMEM(deep, jnp.float32),
            ),
            in_specs=[hbm] * 8,
            out_specs=(vmem, vmem),
            scratch_shapes=[
                pltpu.VMEM((STEPS + 1, depth + 2 * REACH, width + 2 * REACH, length), jnp.float32),
                pltpu.VMEM(sides, jnp.float32),
                pltpu.VMEM(flat, jnp.bfloat16),
                pltpu.VMEM(flat, jnp.float32),
                pltpu.VMEM(flat, jnp.float32),
                pltpu.VMEM((STEPS, width, length), jnp.float32),
                pltpu.VMEM((depth + 2, width, length), jnp.float32),
                pltpu.VMEM(flat, jnp.float32),
                pltpu.VMEM((2 * length, 2 * length), jnp.bfloat16),
                pltpu.SMEM(wavelet.shape, jnp.float32),
                pltpu.VMEM((width, length), jnp.int32),
                pltpu.VMEM((width, length), jnp.int32),
                pltpu.VMEM((width, length), jnp.int32),
                pltpu.SemaphoreType.DMA((8,)),
                pltpu.SemaphoreType.DMA((2,)),
                pltpu.SemaphoreType.DMA((2, parts)),
                pltpu.SemaphoreType.DMA((2, parts, 2) if ny > 1 else (1, 1, 1)),
                pltpu.SemaphoreType.DMA((2, parts, 2) if ny > 1 else (1, 1, 1)),
                pltpu.SemaphoreType.DMA,
                pltpu.SemaphoreType.DMA,
                pltpu.SemaphoreType.REGULAR((max((nx - 1).bit_length(), 1), 2)),
            ],
            compiler_params=pltpu.CompilerParams(
                collective_id=0, has_side_effects=True, vmem_limit_bytes=60000000
            ),
        )(pressure, prior, courant, wavelet, delay, sdepth, rdepth, receiver)
        return pl.pallas_call(
            store,
            out_shape=(
                jax.ShapeDtypeStruct(flat, jnp.float32),
                jax.ShapeDtypeStruct(deep, jnp.float32),
            ),
            in_specs=[vmem] * 2,
            out_specs=(hbm, hbm),
            scratch_shapes=[pltpu.SemaphoreType.DMA((2,))],
            compiler_params=pltpu.CompilerParams(vmem_limit_bytes=4 << 20),
        )(*(pltpu.with_memory_space_constraint(part, pltpu.VMEM) for part in held))

    in_specs = (
        P(None, ("shots", "gx"), "gy"),
        P(None, ("shots", "gx"), "gy"),
        P(None, "gx", "gy"),
        P("shots"),
        P(("shots", "gx"), "gy"),
        P(("shots", "gx"), "gy"),
        P(("shots", "gx"), "gy"),
        P(None, ("shots", "gx"), "gy"),
    )
    out_specs = (P(None, ("shots", "gx"), "gy"), P("gx", "shots", "gy"))
    return jax.shard_map(shards, mesh=mesh, in_specs=in_specs, out_specs=out_specs, check_vma=False)
```

```python
import functools

import jax
import jax.numpy as jnp
from jax import lax
from jax.experimental import pallas as pl
from jax.experimental.pallas import tpu as pltpu
from jax.sharding import PartitionSpec as P

STEPS = 8
REACH = 4
CENTER = -205.0 / 72.0
COEFS = (1.6, -0.2, 8.0 / 315.0, -1.0 / 560.0)
GROUP = 8


def chunks_of(depth):
    quarter = depth // 4
    return tuple((quarter * c, quarter) for c in (0, 2, 1, 3))


def kernel(
    nx,
    ny,
    pressure,
    prior,
    courant,
    wavelet,
    delay,
    sdepth,
    rdepth,
    receiver,
    final,
    image,
    field,
    side,
    courant_v,
    receiver_v,
    partial,
    amp,
    product,
    slab,
    weights,
    wave_v,
    small_v,
    local_sem,
    send_sem,
    recv_sem,
    side_send,
    side_recv,
    img_send,
    img_recv,
    known,
):
    depth, width, length = pressure.shape
    chunks = chunks_of(depth)
    slab_depth = depth // nx
    me = lax.axis_index("gx")
    mine = lax.axis_index("gy")
    own = pl.ds(REACH, width)

    barrier = pltpu.get_barrier_semaphore()

    def toward(way, far):
        return (me + far, me + far < nx) if way == 0 else (me - far, me >= far)

    if nx > 1:
        for way in (0, 1):
            peer, there = toward(way, 1)

            @pl.when(there)
            def _():
                pl.semaphore_signal(
                    barrier,
                    inc=1,
                    device_id={"gx": peer},
                    device_id_type=pl.DeviceIdType.MESH,
                )

    for j in range(1, ny):
        pl.semaphore_signal(
            barrier,
            inc=1,
            device_id={"gy": lax.rem(mine + j, ny)},
            device_id_type=pl.DeviceIdType.MESH,
        )

    local = [
        pltpu.make_async_copy(prior, field.at[0, pl.ds(REACH, depth), own, :], local_sem.at[0]),
        pltpu.make_async_copy(courant, courant_v, local_sem.at[1]),
        pltpu.make_async_copy(wavelet, wave_v, local_sem.at[2]),
        pltpu.make_async_copy(delay, small_v.at[0], local_sem.at[3]),
        pltpu.make_async_copy(sdepth, small_v.at[1], local_sem.at[3]),
        pltpu.make_async_copy(rdepth, small_v.at[2], local_sem.at[3]),
        pltpu.make_async_copy(receiver, receiver_v, local_sem.at[4]),
        pltpu.make_async_copy(pressure, field.at[1, pl.ds(REACH, depth), own, :], local_sem.at[0]),
    ]
    def span(c):
        z, rows = chunks[c]
        return pl.ds(REACH + z, rows)

    def face(t, c, way, opening):
        z, rows = chunks[c]
        source = width - REACH if way == 0 else 0
        target = 0 if way == 0 else REACH + width
        return pltpu.make_async_remote_copy(
            src_ref=pressure.at[pl.ds(z, rows), pl.ds(source, REACH), :]
            if opening
            else field.at[t + 1, span(c), pl.ds(REACH + source, REACH), :],
            dst_ref=field.at[t + 1, span(c), pl.ds(target, REACH), :],
            send_sem=send_sem.at[t % 2],
            recv_sem=recv_sem.at[t % 2, c],
            device_id={"gx": lax.rem(me + (1 if way == 0 else nx - 1), nx)},
            device_id_type=pl.DeviceIdType.MESH,
        )

    def flank(t, c, way, opening):
        peer = lax.rem(mine + 1, ny) if way == 0 else lax.rem(mine + ny - 1, ny)
        z, rows = chunks[c]
        return pltpu.make_async_remote_copy(
            src_ref=pressure.at[pl.ds(z, rows), :, :]
            if opening
            else field.at[t + 1, span(c), own, :],
            dst_ref=side.at[t, way, pl.ds(z, rows), :, :],
            send_sem=side_send.at[t % 2, c, way],
            recv_sem=side_recv.at[t % 2, c, way],
            device_id={"gy": peer},
            device_id_type=pl.DeviceIdType.MESH,
        )

    def send(t, c, opening=False):
        if nx > 1:
            for way in (0, 1):

                @pl.when(me < nx - 1 if way == 0 else me > 0)
                def _():
                    face(t, c, way, opening).start()

        if ny > 1:
            for way in (0, 1):

                @pl.when(mine < ny - 1 if way == 0 else mine > 0)
                def _():
                    flank(t, c, way, opening).start()

    def faces(t, begin, rows, ways, c):
        both = field.at[t + 1, pl.ds(REACH + begin, rows), pl.ds(0, ways * REACH), :]
        return pltpu.make_async_remote_copy(
            src_ref=both,
            dst_ref=both,
            send_sem=send_sem.at[t % 2],
            recv_sem=recv_sem.at[t % 2, c],
            device_id={"gx": lax.rem(me + 1, nx)},
            device_id_type=pl.DeviceIdType.MESH,
        )

    edge = jnp.logical_or(me == 0, me == nx - 1)

    def each_count(act):
        if nx > 1:

            @pl.when(edge)
            def _():
                act(1)

        if nx > 2:

            @pl.when(jnp.logical_not(edge))
            def _():
                act(2)

    def sent(t):
        each_count(lambda ways: faces(t, 0, depth, ways, 0).wait_send())
        if ny > 1:
            for way in (0, 1):

                @pl.when(mine < ny - 1 if way == 0 else mine > 0)
                def _():
                    for c in range(len(chunks)):
                        flank(t, c, way, False).wait_send()

    def arrived(t, c):
        begin, rows = chunks[c]
        each_count(lambda ways: faces(t, begin, rows, ways, c).wait_recv())
        if ny > 1:
            for way in (0, 1):

                @pl.when(mine > 0 if way == 0 else mine < ny - 1)
                def _():
                    flank(t, c, way, False).wait_recv()

    beside = (me > 0).astype(jnp.int32) + (me < nx - 1).astype(jnp.int32)
    if nx > 1 or ny > 1:
        pl.semaphore_wait(barrier, beside + ny - 1)

    for c in range(len(chunks)):
        send(0, c, opening=True)
    for copy in local[::-1]:
        copy.start()

    rim = jnp.zeros((REACH, width + 2 * REACH, length), jnp.float32)
    for t in range(STEPS):
        field[t + 1, pl.ds(0, REACH), :, :] = rim
        field[t + 1, pl.ds(REACH + depth, REACH), :, :] = rim

    def clear(at):
        def one(t, carry):
            field[t + 1, pl.ds(REACH, depth), pl.ds(at, REACH), :] = jnp.zeros(
                (depth, REACH, length), jnp.float32
            )
            return carry

        lax.fori_loop(0, STEPS, one, 0)

    @pl.when(me == 0)
    def _():
        clear(0)

    @pl.when(me == nx - 1)
    def _():
        clear(REACH + width)

    if ny > 1:

        def clear_side(k):
            def one(t, carry):
                side[t, k] = jnp.zeros((depth, width, length), jnp.float32)
                return carry

            lax.fori_loop(0, STEPS, one, 0)

        @pl.when(mine == 0)
        def _():
            clear_side(0)

        @pl.when(mine == ny - 1)
        def _():
            clear_side(1)

    product[pl.ds(0, 1), :, :] = jnp.zeros((1, width, length), jnp.float32)
    product[pl.ds(depth + 1, 1), :, :] = jnp.zeros((1, width, length), jnp.float32)

    start = lax.broadcasted_iota(jnp.int32, (length, length), 0)
    gap = jnp.abs(start - lax.broadcasted_iota(jnp.int32, (length, length), 1))
    band = jnp.where(gap == 0, 3.0 * CENTER, 0.0)
    for k in range(1, REACH + 1):
        band = jnp.where(gap == k, COEFS[k - 1], band)
    band_high = band.astype(jnp.bfloat16)
    band_low = (band - band_high.astype(jnp.float32)).astype(jnp.bfloat16)
    weights[...] = jnp.concatenate(
        [
            jnp.concatenate([band_high, band_low], axis=1),
            jnp.concatenate([band_high, jnp.zeros_like(band_low)], axis=1),
        ],
        axis=0,
    )

    fields = field.at[pl.ds(0, 2), pl.ds(REACH, depth), own, :]
    pltpu.make_async_copy(fields, fields, local_sem.at[0]).wait()
    local[1].wait()
    local[2].wait()
    pltpu.make_async_copy(small_v, small_v, local_sem.at[3]).wait()
    late = small_v[0]
    for t in range(STEPS):
        total = jnp.zeros((width, length), jnp.float32)
        for pick in range(wavelet.shape[0]):
            total = total + jnp.where(late + t == pick, wave_v[pick], 0.0)
        amp[t] = total

    lanes = lax.broadcasted_iota(jnp.int32, (width, length), 1)
    origin = small_v[1]

    def along(v):
        tall = v.reshape(GROUP * width, length)
        high = tall.astype(jnp.bfloat16)
        low = (tall - high.astype(jnp.float32)).astype(jnp.bfloat16)
        both = jnp.dot(
            jnp.concatenate([high, low], axis=1), weights[...], preferred_element_type=jnp.float32
        )
        return (both[:, :length] + both[:, length:]).reshape(GROUP, width, length)

    def prepare(t, z):
        at = t + 1
        v = field[at, pl.ds(REACH + z, GROUP), own, :]
        old = field[t, pl.ds(REACH + z, GROUP), own, :]
        total = (3.0 * CENTER) * v if ny > 1 else along(v)
        for k in range(1, REACH + 1):
            total = total + COEFS[k - 1] * (
                field[at, pl.ds(REACH + z + k, GROUP), own, :]
                + field[at, pl.ds(REACH + z - k, GROUP), own, :]
            )
        strength = courant_v[pl.ds(z, GROUP), :, :].astype(jnp.float32)
        levels = lax.broadcasted_iota(jnp.int32, (GROUP, width, length), 0) + z
        shot = jnp.where(levels == origin[None], amp[t][None], 0.0)
        partial[pl.ds(z, GROUP), :, :] = 2.0 * v - old + strength * total + shot

    def complete(t, z):
        at = t + 1
        total = None
        for k in range(1, REACH + 1):
            near = (
                field[at, pl.ds(REACH + z, GROUP), pl.ds(REACH + k, width), :]
                + field[at, pl.ds(REACH + z, GROUP), pl.ds(REACH - k, width), :]
            )
            if ny > 1:
                v = field[at, pl.ds(REACH + z, GROUP), own, :]
                up = pltpu.roll(v, length - k, 2)
                down = pltpu.roll(v, k, 2)
                low = pltpu.roll(side[t, 0, pl.ds(z, GROUP), :, :], k, 2)
                high = pltpu.roll(side[t, 1, pl.ds(z, GROUP), :, :], length - k, 2)
                up = jnp.where((lanes < length - k)[None], up, high)
                down = jnp.where((lanes >= k)[None], down, low)
                near = near + (up + down)
            total = COEFS[k - 1] * near if k == 1 else total + COEFS[k - 1] * near
        strength = courant_v[pl.ds(z, GROUP), :, :].astype(jnp.float32)
        return partial[pl.ds(z, GROUP), :, :] + strength * total

    def prepared(t, begin, rows):
        def group(g, inner):
            prepare(t, begin + g * GROUP)
            return inner

        lax.fori_loop(0, rows // GROUP, group, 0, unroll=True)

    reach = []
    while (reach[-1] * 2 if reach else 1) < nx:
        reach.append(reach[-1] * 2 if reach else 1)

    def greet(number):
        for way in (0, 1):
            peer, there = toward(way, reach[number])

            @pl.when(there)
            def _():
                pl.semaphore_signal(
                    known.at[number, way],
                    inc=1,
                    device_id={"gx": peer},
                    device_id_type=pl.DeviceIdType.MESH,
                )

    def greeted(number):
        for way in (0, 1):
            there = toward(1 - way, reach[number])[1]

            @pl.when(there)
            def _():
                pl.semaphore_wait(known.at[number, way], 1)

    def meet(number):
        if number > 0:
            greeted(number - 1)
        greet(number)

    def step(t, carry):
        for number in range(len(reach)):
            if number + 1 < STEPS - 1:

                @pl.when(t == number + 1)
                def _():
                    meet(number)

        @pl.when(t > 0)
        def _():
            sent(t - 1)

        for c, (begin, rows) in enumerate(chunks):
            prepared(t, begin, rows)
            arrived(t, c)

            def group(g, inner):
                z = begin + g * GROUP
                field[t + 2, pl.ds(REACH + z, GROUP), own, :] = complete(t, z)
                return inner

            lax.fori_loop(0, rows // GROUP, group, 0, unroll=True)
            send(t + 1, c)
        return carry

    lax.fori_loop(0, STEPS - 1, step, 0)
    for number in range(len(reach)):
        if number + 1 >= STEPS - 1:
            meet(number)
    if reach:
        greeted(len(reach) - 1)

    def landing(who):
        return image.at[:, pl.ds(pl.multiple_of(who * width, width), width), :]

    def piece(peer):
        return pltpu.make_async_remote_copy(
            src_ref=slab.at[pl.ds(peer * slab_depth, slab_depth), :, :],
            dst_ref=landing(me),
            send_sem=img_send,
            recv_sem=img_recv,
            device_id={"gx": peer},
            device_id_type=pl.DeviceIdType.MESH,
        )

    def filtered(peer):
        z = peer * slab_depth
        return (
            2.0 * product[pl.ds(1 + z, slab_depth), :, :]
            - product[pl.ds(z, slab_depth), :, :]
            - product[pl.ds(2 + z, slab_depth), :, :]
        )

    def ship(low, count):
        def one(j, carry):
            peer = low + lax.rem(me + 1 + j, count)
            value = filtered(peer)

            @pl.when(peer != me)
            def _():
                slab[pl.ds(peer * slab_depth, slab_depth), :, :] = value
                piece(peer).start()

            @pl.when(peer == me)
            def _():
                landing(me)[...] = value

            return carry

        lax.fori_loop(0, count, one, 0)

    local[6].wait()
    ground = small_v[2]
    last = STEPS - 1
    ready, gone = set(), set()
    for c, (begin, rows) in enumerate(chunks):
        prepared(last, begin, rows)
        arrived(last, c)

        def group(g, inner):
            z = begin + g * GROUP
            new = complete(last, z)
            final[pl.ds(z, GROUP), :, :] = new
            levels = lax.broadcasted_iota(jnp.int32, (GROUP, width, length), 0) + z
            masked = jnp.where(levels >= ground[None], receiver_v[pl.ds(z, GROUP), :, :], 0.0)
            product[pl.ds(1 + z, GROUP), :, :] = new * masked
            return inner

        lax.fori_loop(0, rows // GROUP, group, 0, unroll=True)
        ready |= set(range(begin, begin + rows))
        able = [
            peer
            for peer in range(nx)
            if peer not in gone
            and all(
                level in ready
                for level in range(
                    max(peer * slab_depth - 1, 0), min((peer + 1) * slab_depth + 1, depth)
                )
            )
        ]
        gone |= set(able)
        low = 0
        while low < len(able):
            high = low + 1
            while high < len(able) and able[high] == able[high - 1] + 1:
                high += 1
            ship(able[low], high - low)
            low = high

    for t in range(max(STEPS - 2, 0), STEPS):
        sent(t)
    if nx > 1:
        others = pltpu.make_async_remote_copy(
            src_ref=slab.at[pl.ds(0, (nx - 1) * slab_depth), :, :],
            dst_ref=image.at[:, pl.ds(0, (nx - 1) * width), :],
            send_sem=img_send,
            recv_sem=img_recv,
            device_id={"gx": lax.rem(me + 1, nx)},
            device_id_type=pl.DeviceIdType.MESH,
        )
        others.wait_send()
        others.wait_recv()


def store(final_v, image_v, final, image, sem):
    copies = (
        pltpu.make_async_copy(final_v, final, sem.at[0]),
        pltpu.make_async_copy(image_v, image, sem.at[1]),
    )
    for copy in copies:
        copy.start()
    for copy in copies:
        copy.wait()


def solution(mesh):
    nx, ny = mesh.shape["gx"], mesh.shape["gy"]

    def shards(pressure, prior, courant, wavelet, delay, sdepth, rdepth, receiver):
        depth, width, length = pressure.shape
        parts = len(chunks_of(depth))
        hbm = pl.BlockSpec(memory_space=pl.ANY)
        vmem = pl.BlockSpec(memory_space=pltpu.VMEM)
        flat = (depth, width, length)
        sides = (STEPS, 2, depth, width, length) if ny > 1 else (1, 1, 1, width, length)
        deep = (depth // nx, width * nx, length)
        held = pl.pallas_call(
            functools.partial(kernel, nx, ny),
            out_shape=(
                pltpu.VMEM(flat, jnp.float32),
                pltpu.VMEM(deep, jnp.float32),
            ),
            in_specs=[hbm] * 8,
            out_specs=(vmem, vmem),
            scratch_shapes=[
                pltpu.VMEM((STEPS + 1, depth + 2 * REACH, width + 2 * REACH, length), jnp.float32),
                pltpu.VMEM(sides, jnp.float32),
                pltpu.VMEM(flat, jnp.bfloat16),
                pltpu.VMEM(flat, jnp.float32),
                pltpu.VMEM(flat, jnp.float32),
                pltpu.VMEM((STEPS, width, length), jnp.float32),
                pltpu.VMEM((depth + 2, width, length), jnp.float32),
                pltpu.VMEM(flat, jnp.float32),
                pltpu.VMEM((2 * length, 2 * length), jnp.bfloat16),
                pltpu.SMEM(wavelet.shape, jnp.float32),
                pltpu.VMEM((3, width, length), jnp.int32),
                pltpu.SemaphoreType.DMA((5,)),
                pltpu.SemaphoreType.DMA((2,)),
                pltpu.SemaphoreType.DMA((2, parts)),
                pltpu.SemaphoreType.DMA((2, parts, 2) if ny > 1 else (1, 1, 1)),
                pltpu.SemaphoreType.DMA((2, parts, 2) if ny > 1 else (1, 1, 1)),
                pltpu.SemaphoreType.DMA,
                pltpu.SemaphoreType.DMA,
                pltpu.SemaphoreType.REGULAR((max((nx - 1).bit_length(), 1), 2)),
            ],
            compiler_params=pltpu.CompilerParams(
                collective_id=0, has_side_effects=True, vmem_limit_bytes=60000000
            ),
        )(pressure, prior, courant, wavelet, delay, sdepth, rdepth, receiver)
        return pl.pallas_call(
            store,
            out_shape=(
                jax.ShapeDtypeStruct(flat, jnp.float32),
                jax.ShapeDtypeStruct(deep, jnp.float32),
            ),
            in_specs=[vmem] * 2,
            out_specs=(hbm, hbm),
            scratch_shapes=[pltpu.SemaphoreType.DMA((2,))],
            compiler_params=pltpu.CompilerParams(vmem_limit_bytes=4 << 20),
        )(*(pltpu.with_memory_space_constraint(part, pltpu.VMEM) for part in held))

    in_specs = (
        P(None, ("shots", "gx"), "gy"),
        P(None, ("shots", "gx"), "gy"),
        P(None, "gx", "gy"),
        P("shots"),
        P(("shots", "gx"), "gy"),
        P(("shots", "gx"), "gy"),
        P(("shots", "gx"), "gy"),
        P(None, ("shots", "gx"), "gy"),
    )
    out_specs = (P(None, ("shots", "gx"), "gy"), P("gx", "shots", "gy"))
    return jax.shard_map(shards, mesh=mesh, in_specs=in_specs, out_specs=out_specs, check_vma=False)
```
